256 devices in a mesh: row: 16 (over x, y), col: 16 (over z, core).
Axes of the slice: x: 4, y: 4, z: 8, core: 2. Of those that a mesh axis runs over, the one named last changes fastest.
Arguments:
- panel: float32 [49152, 512], P(('row', 'col')), may hold values from -0.027063294 to 0.027063294
- trailing: float32 [49152, 8192], P('row', 'col'), may hold values from -6 to 6
- counts: int32 [16], P('row'), may hold values from 1 to 6, 56 in all
Outputs:
- upper: float32 [512, 512], replicated
- projected: float32 [512, 8192], P(None, 'col')
The draws below stay inside these ranges and needn't reach their ends.
Inputs may be any that keep to these rules, and one draw needn't show every extreme that they name: `counts`: the valid tiles of a block are its first ones; some grid row has all 6 valid.
All inputs are finite; a program needn't handle non-finite values.
Results may differ from the reference program's by a relative error of at most 0.0003.
Values sent between devices are 32-bit elements; how exact they have to be, the bound alone decides.
No kernel may reach another device: no remote copies, remote signals or barrier semaphores. Data moves between devices by JAX's collectives and lax.ppermute only.
A program may use at most 64 MiB of HBM per device.

```python
import math
import jax
import jax.numpy as jnp
import numpy as np
from jax import lax

B = 512
TILES_DEV = 6
ROWS = 49152
NC = 8192
N_ROW = 16


def draw_panel(key, part):
    base = jax.random.fold_in(key, 11)
    key_own, key_shared = jax.random.split(base, 2)
    share = 0.02
    own = jax.random.normal(key_own, (ROWS, B), jnp.float32)
    shared = jax.random.normal(key_shared, (ROWS, 1), jnp.float32)
    values = math.sqrt(1.0 - share) * own + math.sqrt(share) * shared
    values = jnp.clip(values, -6.0, 6.0) * float(ROWS) ** (-0.5)
    return values.astype(jnp.float32)


def levels(rng, shape, shards, low, largest):
    def one(axis_at, shards_of):
        draws = jax.random.uniform(jax.random.fold_in(jax.random.fold_in(rng, 6), axis_at), (shards_of,), jnp.float32, low / len(shards), largest / len(shards))
        return jnp.repeat(jnp.exp(draws), shape[axis_at] // shards_of).reshape((-1,) + (1,) * (len(shape) - axis_at - 1))

    loudness = one(*shards[0])
    for cut in shards[1:]:
        loudness = loudness * one(*cut)
    return loudness


def length_profile(number_of, total, limit, slope):
    weights = [(1 << 20) // math.isqrt(grade ** slope) + 1 for grade in range(2, number_of + 1)]
    rest, given = total - limit - (number_of - 1), [1] * (number_of - 1)
    while rest > 0:
        free = [i for i in range(number_of - 1) if given[i] < limit]
        whole, remaining = sum([weights[i] for i in free]), rest
        for i in free:
            extra = min(limit - given[i], max(1, remaining * weights[i] // whole), rest)
            given[i] = given[i] + extra
            rest = rest - extra
    return np.array([limit] + given)


def uneven_parts(key, number_of, total, bound, skew):
    if number_of == 2:
        one = jax.random.randint(key, (), max(1, total - bound), min(bound, total - 1) + 1)
        return jnp.stack([one, total - one])
    tallies = jnp.asarray(length_profile(number_of, total, bound, skew), jnp.int32)
    couples = (number_of - 1) // 2
    donor, receiver = tallies[1:1 + 2 * couples:2], tallies[2:2 + 2 * couples:2]
    room = jnp.minimum(donor - 1, bound - receiver)
    passed = jax.random.randint(jax.random.fold_in(key, 1), (couples,), 0, 1 << 20) % (room + 1)
    tallies = tallies.at[1:1 + 2 * couples:2].set(donor - passed).at[2:2 + 2 * couples:2].set(receiver + passed)
    return tallies[jax.random.permutation(jax.random.fold_in(key, 2), number_of)]


def centred(own_key, extent, scale, reach, shards=(), held_as=jnp.bfloat16):
    factor_of = levels(own_key, extent, shards, -0.22, 0.18) if shards else 1.0
    array = jax.random.normal(own_key, extent, jnp.float32) * scale * factor_of
    return jnp.minimum(jnp.maximum(array, -reach), reach).astype(held_as)


def setup_inputs(seed: int = 0) -> dict:
    seeds = jax.random.split(jax.random.key(seed), 4)
    panel = draw_panel(jax.random.fold_in(seeds[3], 71), 0)
    trailing = centred(seeds[1], (ROWS, NC), 1.0, 6.0, ((0, 16), (1, 16)), jnp.float32)
    counts = uneven_parts(seeds[2], N_ROW, (TILES_DEV + 1) * N_ROW // 2, TILES_DEV, 0).astype(jnp.int32)
    return {"panel": panel, "trailing": trailing, "counts": counts}


def reference(panel, trailing, counts):
    width = panel.shape[1]
    indices = lax.iota(jnp.int32, ROWS)
    block = indices // (TILES_DEV * width)
    tile = indices % (TILES_DEV * width) // width
    keep = (tile < counts[block]).astype(jnp.float32)
    masked = panel * keep[:, None]
    factor_q, factor_r = jnp.linalg.qr(masked)
    signs = jnp.sign(jnp.diagonal(factor_r))
    upper = signs[:, None] * factor_r
    projected = signs[:, None] * jnp.dot(factor_q.T.astype(jnp.float32), trailing.astype(jnp.float32), precision=lax.Precision.HIGHEST, preferred_element_type=jnp.float32)
    return (upper, projected)
```

```python
import functools

import jax
import jax.numpy as jnp
from jax import lax
from jax.experimental import pallas as pl
from jax.experimental.pallas import tpu as pltpu
from jax.sharding import PartitionSpec as P

HIGHEST = lax.Precision.HIGHEST
VMEM = pl.BlockSpec(memory_space=pltpu.VMEM)
SMEM = pl.BlockSpec(memory_space=pltpu.SMEM)
BLOCK = 128


def exact_dot(left, right):
    return lax.dot_general(
        left, right, (((1,), (0,)), ((), ())), precision=HIGHEST, preferred_element_type=jnp.float32
    )


def split(value):
    high = value.astype(jnp.bfloat16)
    return high, (value - high.astype(jnp.float32)).astype(jnp.bfloat16)


def upper_blocks(width):
    count = width // BLOCK
    return [(i, j) for i in range(count) for j in range(i, count)]


def gram_kernel(place_ref, panel_ref, out_ref):
    rows, width = panel_ref.shape
    index = place_ref[0] * rows + lax.broadcasted_iota(jnp.int32, (rows, 1), 0)
    masked = jnp.where(index < place_ref[1] * width, panel_ref[...], 0.0)
    flipped = masked.T
    at = 0
    for i in range(width // BLOCK):
        start = i * BLOCK
        strip = exact_dot(flipped[start : start + BLOCK, :], masked[:, start:])
        for j in range((width - start) // BLOCK):
            out_ref[at : at + BLOCK, :] = strip[:, j * BLOCK : (j + 1) * BLOCK]
            at += BLOCK


def gram(place, panel):
    blocks = len(upper_blocks(panel.shape[1]))
    return pl.pallas_call(
        gram_kernel,
        out_shape=jax.ShapeDtypeStruct((blocks * BLOCK, BLOCK), jnp.float32),
        in_specs=[SMEM, VMEM],
        out_specs=VMEM,
        name="gram",
    )(place, panel)


def eliminate(e):
    rows = len(e)
    sub = lax.broadcasted_iota(jnp.int32, e[0].shape, 0)
    for g in range(rows):
        cols = [[None] * rows for _ in range(8)]
        for j in range(8):
            for v in range(g, rows):
                at = 8 * g + j
                cols[j][v] = jnp.broadcast_to(e[v][:, at : at + 1], (8, 128))
        for k in range(8):
            scale = lax.rsqrt(cols[k][g][k : k + 1, :])
            wide = jnp.concatenate([scale] * (e[0].shape[1] // 128), axis=1)
            pivot = e[g][k : k + 1, :] * wide
            tops = [cols[j][g][k : k + 1, :] * scale for j in range(k + 1, 8)]
            for v in range(g, rows):
                m = cols[k][v] * scale
                if v == g:
                    m = jnp.where(sub[:, :128] > k, m, 0.0)
                    e[v] = jnp.where(sub == k, pivot, e[v])
                many = jnp.concatenate([m] * (e[0].shape[1] // 128), axis=1)
                e[v] = e[v] - many * pivot
                for j in range(k + 1, 8):
                    cols[j][v] = cols[j][v] - m * tops[j - k - 1]
    return e


def factor_kernel(packed_ref, upper_ref, inverse_ref):
    width = upper_ref.shape[0]
    count = width // BLOCK
    work = {}
    for at, key in enumerate(upper_blocks(width)):
        work[key] = packed_ref[at * BLOCK : (at + 1) * BLOCK, :]
    upper_ref[...] = jnp.zeros_like(upper_ref)
    inverse_ref[...] = jnp.zeros_like(inverse_ref)
    row = lax.broadcasted_iota(jnp.int32, (BLOCK, BLOCK), 0)
    column = lax.broadcasted_iota(jnp.int32, (BLOCK, BLOCK), 1)
    eye = (row == column).astype(jnp.float32)
    for s in range(count):
        here = slice(s * BLOCK, (s + 1) * BLOCK)
        if s == 0:
            diagonal = packed_ref[:BLOCK, :]
        else:
            diagonal = work_diagonal
        both = jnp.concatenate([diagonal, eye], axis=1)
        both = jnp.concatenate(eliminate([both[8 * v : 8 * v + 8, :] for v in range(BLOCK // 8)]), axis=0)
        inverse = both[:, BLOCK:]
        upper_ref[here, here] = jnp.where(row <= column, both[:, :BLOCK], 0.0)
        left = None
        if s:
            left = exact_dot(inverse, inverse_ref[here, : s * BLOCK])
            inverse_ref[here, : s * BLOCK] = left
        inverse_ref[here, here] = inverse
        if s + 1 < count:
            strip = jnp.concatenate([work[s, j] for j in range(s + 1, count)], axis=1)
            strip = exact_dot(inverse, strip)
            upper_ref[here, (s + 1) * BLOCK :] = strip
            flipped = strip.T
            for i in range(s + 1, count):
                part = flipped[(i - s - 1) * BLOCK : (i - s) * BLOCK, :]
                change = exact_dot(part, strip[:, (i - s - 1) * BLOCK :])
                for j in range(i, count):
                    work[i, j] = work[i, j] - change[:, (j - i) * BLOCK : (j - i + 1) * BLOCK]
                there = slice(i * BLOCK, (i + 1) * BLOCK)
                inverse_ref[there, here] = -exact_dot(part, inverse)
                if s:
                    inverse_ref[there, : s * BLOCK] -= exact_dot(part, left)
            work_diagonal = work[s + 1, s + 1]


def factor(packed, width):
    return pl.pallas_call(
        factor_kernel,
        out_shape=[jax.ShapeDtypeStruct((width, width), jnp.float32)] * 2,
        in_specs=[VMEM],
        out_specs=[VMEM, VMEM],
        cost_estimate=pl.CostEstimate(flops=20_000_000_000, bytes_accessed=3 << 20, transcendentals=512),
        name="factor",
    )(packed)


def cross_kernel(valid_ref, piece_ref, trailing_ref, out_ref):
    step = pl.program_id(0)

    @pl.when(step == 0)
    def _():
        out_ref[...] = jnp.zeros_like(out_ref)

    @pl.when(step < valid_ref[0])
    def _():
        left = split(piece_ref[...])
        right = split(trailing_ref[...])

        def product(a, b):
            return lax.dot_general(a, b, (((0,), (0,)), ((), ())), preferred_element_type=jnp.float32)

        out_ref[...] += product(left[0], right[0]) + (product(left[0], right[1]) + product(left[1], right[0]))


def cross(valid, piece, trailing):
    rows, width = piece.shape
    columns = trailing.shape[1]
    return pl.pallas_call(
        cross_kernel,
        grid=(rows // width,),
        out_shape=jax.ShapeDtypeStruct((width, columns), jnp.float32),
        in_specs=[
            SMEM,
            pl.BlockSpec((width, width), lambda i: (i, 0)),
            pl.BlockSpec((width, columns), lambda i: (i, 0)),
        ],
        out_specs=pl.BlockSpec((width, columns), lambda i: (0, 0)),
        name="cross",
    )(valid, piece, trailing)


def apply_kernel(inverse_ref, total_ref, out_ref):
    width = inverse_ref.shape[0]
    right = split(total_ref[...])
    for i in range(width // BLOCK):
        here, known = slice(i * BLOCK, (i + 1) * BLOCK), (i + 1) * BLOCK
        left = split(inverse_ref[here, :known])

        def product(a, b):
            return lax.dot_general(a, b[:known, :], (((1,), (0,)), ((), ())), preferred_element_type=jnp.float32)

        out_ref[here, :] = product(left[0], right[0]) + (product(left[0], right[1]) + product(left[1], right[0]))


def apply(inverse, total):
    return pl.pallas_call(
        apply_kernel,
        out_shape=jax.ShapeDtypeStruct(total.shape, jnp.float32),
        in_specs=[VMEM, VMEM],
        out_specs=VMEM,
        name="apply",
    )(inverse, total)


def exchange(blocks, axis, groups=None):
    return lax.all_to_all(blocks, axis, 0, 0, tiled=True, axis_index_groups=groups)


def spread(block, count):
    return jnp.broadcast_to(block[None], (count, *block.shape))


def body(rows, cols, panel, trailing, counts):
    width = panel.shape[1]
    place = jnp.stack([lax.axis_index("col"), counts[0]])
    piece = lax.all_gather(panel, "col", axis=0, tiled=True)

    lines = cols // 2
    planes = [[r * cols + 2 * z + k for r in range(rows) for k in range(2)] for z in range(lines)]
    uprights = [[2 * z + k for z in range(lines)] for k in range(2)]
    both = ("row", "col")
    packed = gram(place, panel)
    shares = exchange(packed.reshape(2 * rows, -1, BLOCK), both, planes)
    shares = jnp.sum(shares, axis=0)
    shares = jnp.sum(exchange(spread(shares, lines), "col", uprights), axis=0)
    packed = exchange(spread(shares, 2 * rows), both, planes).reshape(packed.shape)
    upper, inverse = factor(packed, width)

    total = cross(counts, piece, trailing)
    total = jnp.sum(exchange(total.reshape(rows, -1, total.shape[1]), "row"), axis=0)
    total = exchange(spread(total, rows), "row").reshape(width, -1)
    return upper, apply(inverse, total)


def solution(mesh):
    return jax.shard_map(
        functools.partial(body, mesh.shape["row"], mesh.shape["col"]),
        mesh=mesh,
        in_specs=(P(("row", "col"), None), P("row", "col"), P("row")),
        out_specs=(P(), P(None, "col")),
        check_vma=False,
    )
```

```python
import functools

import jax
import jax.numpy as jnp
from jax import lax
from jax.experimental import pallas as pl
from jax.experimental.pallas import tpu as pltpu
from jax.sharding import PartitionSpec as P

HIGHEST = lax.Precision.HIGHEST
VMEM = pl.BlockSpec(memory_space=pltpu.VMEM)
SMEM = pl.BlockSpec(memory_space=pltpu.SMEM)
BLOCK = 128


def exact_dot(left, right):
    return lax.dot_general(
        left, right, (((1,), (0,)), ((), ())), precision=HIGHEST, preferred_element_type=jnp.float32
    )


def split(value):
    high = value.astype(jnp.bfloat16)
    return high, (value - high.astype(jnp.float32)).astype(jnp.bfloat16)


def upper_blocks(width):
    count = width // BLOCK
    return [(i, j) for i in range(count) for j in range(i, count)]


def gram_kernel(place_ref, panel_ref, out_ref):
    rows, width = panel_ref.shape
    index = place_ref[0] * rows + lax.broadcasted_iota(jnp.int32, (rows, 1), 0)
    masked = jnp.where(index < place_ref[1] * width, panel_ref[...], 0.0)
    flipped = masked.T
    at = 0
    for i in range(width // BLOCK):
        start = i * BLOCK
        strip = exact_dot(flipped[start : start + BLOCK, :], masked[:, start:])
        for j in range((width - start) // BLOCK):
            out_ref[at : at + BLOCK, :] = strip[:, j * BLOCK : (j + 1) * BLOCK]
            at += BLOCK


def gram(place, panel):
    blocks = len(upper_blocks(panel.shape[1]))
    return pl.pallas_call(
        gram_kernel,
        out_shape=jax.ShapeDtypeStruct((blocks * BLOCK, BLOCK), jnp.float32),
        in_specs=[SMEM, VMEM],
        out_specs=VMEM,
        name="gram",
    )(place, panel)


def eliminate(e):
    rows = len(e)
    sub = lax.broadcasted_iota(jnp.int32, e[0].shape, 0)
    for g in range(rows):
        cols = [[None] * rows for _ in range(8)]
        for j in range(8):
            for v in range(g, rows):
                at = 8 * g + j
                cols[j][v] = jnp.broadcast_to(e[v][:, at : at + 1], (8, 128))
        for k in range(8):
            scale = lax.rsqrt(cols[k][g][k : k + 1, :])
            wide = jnp.concatenate([scale] * (e[0].shape[1] // 128), axis=1)
            pivot = e[g][k : k + 1, :] * wide
            tops = [cols[j][g][k : k + 1, :] * scale for j in range(k + 1, 8)]
            for v in range(g, rows):
                m = cols[k][v] * scale
                if v == g:
                    m = jnp.where(sub[:, :128] > k, m, 0.0)
                    e[v] = jnp.where(sub == k, pivot, e[v])
                many = jnp.concatenate([m] * (e[0].shape[1] // 128), axis=1)
                e[v] = e[v] - many * pivot
                for j in range(k + 1, 8):
                    cols[j][v] = cols[j][v] - m * tops[j - k - 1]
    return e


def factor_kernel(packed_ref, upper_ref, inverse_ref):
    width = upper_ref.shape[0]
    count = width // BLOCK
    work = {}
    for at, key in enumerate(upper_blocks(width)):
        work[key] = packed_ref[at * BLOCK : (at + 1) * BLOCK, :]
    upper_ref[...] = jnp.zeros_like(upper_ref)
    inverse_ref[...] = jnp.zeros_like(inverse_ref)
    row = lax.broadcasted_iota(jnp.int32, (BLOCK, BLOCK), 0)
    column = lax.broadcasted_iota(jnp.int32, (BLOCK, BLOCK), 1)
    eye = (row == column).astype(jnp.float32)
    for s in range(count):
        here = slice(s * BLOCK, (s + 1) * BLOCK)
        if s == 0:
            diagonal = packed_ref[:BLOCK, :]
        else:
            diagonal = work_diagonal
        both = jnp.concatenate([diagonal, eye], axis=1)
        both = jnp.concatenate(eliminate([both[8 * v : 8 * v + 8, :] for v in range(BLOCK // 8)]), axis=0)
        inverse = both[:, BLOCK:]
        upper_ref[here, here] = jnp.where(row <= column, both[:, :BLOCK], 0.0)
        left = None
        if s:
            left = exact_dot(inverse, inverse_ref[here, : s * BLOCK])
            inverse_ref[here, : s * BLOCK] = left
        inverse_ref[here, here] = inverse
        if s + 1 < count:
            strip = jnp.concatenate([work[s, j] for j in range(s + 1, count)], axis=1)
            strip = exact_dot(inverse, strip)
            upper_ref[here, (s + 1) * BLOCK :] = strip
            flipped = strip.T
            for i in range(s + 1, count):
                part = flipped[(i - s - 1) * BLOCK : (i - s) * BLOCK, :]
                change = exact_dot(part, strip[:, (i - s - 1) * BLOCK :])
                for j in range(i, count):
                    work[i, j] = work[i, j] - change[:, (j - i) * BLOCK : (j - i + 1) * BLOCK]
                there = slice(i * BLOCK, (i + 1) * BLOCK)
                inverse_ref[there, here] = -exact_dot(part, inverse)
                if s:
                    inverse_ref[there, : s * BLOCK] -= exact_dot(part, left)
            work_diagonal = work[s + 1, s + 1]


def factor(packed, width):
    return pl.pallas_call(
        factor_kernel,
        out_shape=[jax.ShapeDtypeStruct((width, width), jnp.float32)] * 2,
        in_specs=[VMEM],
        out_specs=[VMEM, VMEM],
        cost_estimate=pl.CostEstimate(flops=20_000_000_000, bytes_accessed=3 << 20, transcendentals=512),
        name="factor",
    )(packed)


def cross_kernel(valid_ref, piece_ref, trailing_ref, out_ref):
    step = pl.program_id(0)

    @pl.when(step == 0)
    def _():
        out_ref[...] = jnp.zeros_like(out_ref)

    @pl.when(step < valid_ref[0])
    def _():
        left = split(piece_ref[...])
        right = split(trailing_ref[...])

        def product(a, b):
            return lax.dot_general(a, b, (((0,), (0,)), ((), ())), preferred_element_type=jnp.float32)

        out_ref[...] += product(left[0], right[0]) + (product(left[0], right[1]) + product(left[1], right[0]))


def cross(valid, piece, trailing):
    rows, width = piece.shape
    columns = trailing.shape[1]
    return pl.pallas_call(
        cross_kernel,
        grid=(rows // width,),
        out_shape=jax.ShapeDtypeStruct((width, columns), jnp.float32),
        in_specs=[
            SMEM,
            pl.BlockSpec((width, width), lambda i: (i, 0)),
            pl.BlockSpec((width, columns), lambda i: (i, 0)),
        ],
        out_specs=pl.BlockSpec((width, columns), lambda i: (0, 0)),
        name="cross",
    )(valid, piece, trailing)


def apply_kernel(inverse_ref, total_ref, out_ref):
    width = inverse_ref.shape[0]
    right = split(total_ref[...])
    for i in range(width // BLOCK):
        here, known = slice(i * BLOCK, (i + 1) * BLOCK), (i + 1) * BLOCK
        left = split(inverse_ref[here, :known])

        def product(a, b):
            return lax.dot_general(a, b[:known, :], (((1,), (0,)), ((), ())), preferred_element_type=jnp.float32)

        out_ref[here, :] = product(left[0], right[0]) + (product(left[0], right[1]) + product(left[1], right[0]))


def apply(inverse, total):
    return pl.pallas_call(
        apply_kernel,
        out_shape=jax.ShapeDtypeStruct(total.shape, jnp.float32),
        in_specs=[VMEM, VMEM],
        out_specs=VMEM,
        name="apply",
    )(inverse, total)


def exchange(blocks, axis, groups=None):
    return lax.all_to_all(blocks, axis, 0, 0, tiled=True, axis_index_groups=groups)


def spread(block, count):
    return jnp.broadcast_to(block[None], (count, *block.shape))


def body(rows, cols, panel, trailing, counts):
    width = panel.shape[1]
    place = jnp.stack([lax.axis_index("col"), counts[0]])
    piece = lax.all_gather(panel, "col", axis=0, tiled=True)

    lines = cols // 2
    planes = [[r * cols + 2 * z + k for r in range(rows) for k in range(2)] for z in range(lines)]
    uprights = [[2 * z + k for z in range(lines)] for k in range(2)]
    both = ("row", "col")
    packed = gram(place, panel)
    shares = exchange(packed.reshape(2 * rows, -1, BLOCK), both, planes)
    shares = jnp.sum(shares, axis=0)
    shares = jnp.sum(exchange(spread(shares, lines), "col", uprights), axis=0)
    packed = exchange(spread(shares, 2 * rows), both, planes).reshape(packed.shape)
    piece, packed = lax.optimization_barrier((piece, packed))
    upper, inverse = factor(packed, width)

    total = cross(counts, piece, trailing)
    total = jnp.sum(exchange(total.reshape(rows, -1, total.shape[1]), "row"), axis=0)
    total = exchange(spread(total, rows), "row").reshape(width, -1)
    return upper, apply(inverse, total)


def solution(mesh):
    return jax.shard_map(
        functools.partial(body, mesh.shape["row"], mesh.shape["col"]),
        mesh=mesh,
        in_specs=(P(("row", "col"), None), P("row", "col"), P("row")),
        out_specs=(P(), P(None, "col")),
        check_vma=False,
    )
```
